256 devices in a mesh: kpt: 128 (over x, z, y_hi, core), band: 2 (over y_lo).
Axes of the slice: x: 4, y: 4 (y_hi: 2, y_lo: 2; y = y_hi * 2 + y_lo), z: 8, core: 2. Of those that a mesh axis runs over, the one named last changes fastest.
Arguments:
- margins: bfloat16 [128, 12, 400, 800], P('kpt', None, 'band'), may hold values from -0.21875 to 0.21875
- subspace: bfloat16 [128, 400, 512], P('kpt', 'band'), may hold values from -6 to 6
- shell_weights: float32 [12], replicated, may hold values from 0.3 to 3
- window_count: int32 [128], P('kpt'), may hold values from 200 to 400
Outputs:
- new_subspace: float32 [128, 400, 512], P('kpt', 'band')
The draws below stay inside these ranges and needn't reach their ends.
Inputs may be any that keep to these rules, and one draw needn't show every extreme that they name: window_count[k] is the number of leading bands of k-point k inside its outer window; the other rows up to 400 are padding.
All inputs are finite; a program needn't handle non-finite values.
Results may differ from the reference program's by a relative error of at most 0.0025.
Values may be sent and summed in bfloat16 or wider, within the bound.
A program may use at most 64 MiB of HBM per device.

```python
import math
import jax
import jax.numpy as jnp
import numpy as np
from jax import lax

NB = 400
NW = 256
NBV = 12
SWEEPS = 2
KX = 4
KY = 4
KZ = 8
K = 128


def plant(result, key, least, largest):
    dims = result.shape
    spot = [jax.random.randint(jax.random.fold_in(key, axis), (), 0, dims[axis]) for axis in range(len(dims))]
    result = result.at[tuple(spot)].set(least)
    longest = dims.index(max(dims))
    spot[longest] = (spot[longest] + 1) % dims[longest]
    return result.at[tuple(spot)].set(largest)


def levels(own_key, dims, split, smallest, high):
    def one(dim, parts):
        draws = jax.random.uniform(jax.random.fold_in(jax.random.fold_in(own_key, 6), dim), (parts,), jnp.float32, smallest / len(split), high / len(split))
        return jnp.repeat(jnp.exp(draws), dims[dim] // parts).reshape((-1,) + (1,) * (len(dims) - dim - 1))

    loudness = one(*split[0])
    for cut in split[1:]:
        loudness = loudness * one(*cut)
    return loudness


def gaussian(rng, dims, scale, most, pieces=(), kind=jnp.bfloat16):
    drawn = jax.random.normal(rng, dims, jnp.float32) * scale
    if len(pieces) > 0:
        drawn = levels(rng, dims, pieces, -0.22, 0.18) * drawn
    return jnp.clip(drawn, min=-most, max=most).astype(kind)


def setup_inputs(seed: int = 0) -> dict:
    splits = jax.random.split(jax.random.key(seed), 5)
    return {
        "margins": gaussian(splits[0], (K, NBV, NB, 2 * NB), (2 * NB) ** -0.5, 0.21875, ((0, 128), (2, 2))),
        "subspace": gaussian(splits[1], (K, NB, 2 * NW), 1.0, 6.0, ((0, 128), (1, 2))),
        "shell_weights": jnp.clip(jnp.exp(jax.random.uniform(splits[2], (NBV,), jnp.float32, math.log(0.3), math.log(3.0))), 0.3, 3.0),
        "window_count": plant(jax.random.randint(splits[3], (K,), NB // 2, NB + 1), jax.random.fold_in(splits[3], 1), NB // 2, NB).astype(jnp.int32),
    }


SHELL_VECTORS = ((1, 1, 0), (1, -1, 0), (-1, 1, 0), (-1, -1, 0), (1, 0, 1), (1, 0, -1), (-1, 0, 1), (-1, 0, -1), (0, 1, 1), (0, 1, -1), (0, -1, 1), (0, -1, -1))

def neighbour_table(size_x, size_y, size_z):
    lookup = np.zeros((size_x * size_y * size_z, len(SHELL_VECTORS)), np.int32)
    for place_x in range(size_x):
        for place_y in range(size_y):
            for place_z in range(size_z):
                flat_index = (place_x * size_y + place_y) * size_z + place_z
                for column, shell in enumerate(SHELL_VECTORS):
                    target_x = (place_x + shell[0]) % size_x
                    target_y = (place_y + shell[1]) % size_y
                    target_z = (place_z + shell[2]) % size_z
                    lookup[flat_index, column] = (target_x * size_y + target_y) * size_z + target_z
    return lookup

def stack_complex(matrix, half_cols):
    real_part = matrix[..., :half_cols]
    imag_part = matrix[..., half_cols:]
    upper_half = jnp.concatenate([real_part, imag_part], axis=-1)
    lower_half = jnp.concatenate([-imag_part, real_part], axis=-1)
    return jnp.concatenate([upper_half, lower_half], axis=-2)

def gram_parts(iterate, half_cols):
    blocks = jnp.dot(iterate.T, iterate, precision=lax.Precision.HIGHEST)
    real_part = blocks[:half_cols, :half_cols] + blocks[half_cols:, half_cols:]
    imag_part = blocks[:half_cols, half_cols:] - blocks[half_cols:, :half_cols]
    return jnp.concatenate([real_part, imag_part], axis=1)

def sweep_step(iterate, gram_sum, half_cols):
    identity = jnp.eye(half_cols, dtype=jnp.float32)
    factor = jnp.concatenate([1.5 * identity - 0.5 * gram_sum[:, :half_cols], -0.5 * gram_sum[:, half_cols:]], axis=1)
    return jnp.dot(iterate, stack_complex(factor, half_cols), precision=lax.Precision.HIGHEST)

def assemble(mine, whole, weights, half_cols):
    real_part = mine[..., :half_cols]
    imag_part = mine[..., half_cols:]
    left_rows = jnp.concatenate([mine, jnp.concatenate([imag_part, -real_part], axis=-1)], axis=-2)
    products = jnp.einsum('brc,bsc->brs', left_rows.astype(jnp.float32), whole.astype(jnp.float32), precision=lax.Precision.HIGHEST)
    summed = jnp.einsum('b,brs->rs', weights, products, precision=lax.Precision.HIGHEST)
    row_count = mine.shape[-2]
    return jnp.concatenate([summed[:row_count], summed[row_count:]], axis=1)

def reference(margins, subspace, shell_weights, window_count):
    lookup = jnp.asarray(neighbour_table(KX, KY, KZ)).astype(jnp.int32)
    row_index = lax.iota(jnp.int32, NB)

    def one_point(payload):
        margin, window, targets, current = payload
        nearby = jnp.take(subspace, targets, axis=0)
        products = jnp.einsum('brc,bcs->brs', margin.astype(jnp.float32), stack_complex(nearby, NW).astype(jnp.float32), precision=lax.Precision.HIGHEST)
        projected = jnp.where((row_index < window)[None, :, None], products, 0.0).astype(jnp.bfloat16)
        assembled = assemble(projected, projected, shell_weights, NW)
        iterate = jnp.dot(assembled, stack_complex(current.astype(jnp.float32), NW), precision=lax.Precision.HIGHEST)
        squares = jnp.sum(iterate * iterate)
        iterate = iterate * lax.rsqrt(2.0 * squares / NW + 1e-06)
        for sweep_number in range(SWEEPS):
            iterate = sweep_step(iterate, gram_parts(iterate, NW), NW)
        return iterate * math.sqrt(NB)
    return lax.map(one_point, (margins, window_count, lookup, subspace))
```

```python
import functools
import math

import jax
import jax.numpy as jnp
from jax import lax
from jax.experimental import pallas as pl
from jax.experimental.pallas import tpu as pltpu
from jax.sharding import PartitionSpec as P

SIZE_X, SIZE_Y, SIZE_Z = 4, 4, 8
ROWS = 200
PAD = 208
DEEP = 256
COLS = 512
HALF = 256
SHELL = 12
MESH = pl.DeviceIdType.MESH
F32 = jnp.float32
BF16 = jnp.bfloat16


def dot(a, b):
    return jnp.dot(a, b, preferred_element_type=F32)


def dot_nt(a, b):
    return lax.dot_general(a, b, (((1,), (1,)), ((), ())), preferred_element_type=F32)


def dot_tn(a, b):
    return lax.dot_general(a, b, (((0,), (0,)), ((), ())), preferred_element_type=F32)


def halves(a):
    high = a.astype(BF16)
    return high, (a - high.astype(F32)).astype(BF16)


def dot3(a, b, product=dot):
    a_high, a_low = halves(a)
    b_high, b_low = halves(b)
    return product(a_high, b_high) + (product(a_high, b_low) + product(a_low, b_high))


def complex_rows(both, rows, start):
    upper, lower = both[:rows], both[start:start + rows]
    return jnp.concatenate(
        [upper[:, :HALF] - lower[:, HALF:], upper[:, HALF:] + lower[:, :HALF]], axis=1
    )


def stack_complex(real, imag):
    return jnp.concatenate(
        [jnp.concatenate([real, imag], axis=1), jnp.concatenate([-imag, real], axis=1)], axis=0
    )


def kernel(
    window_ref, weight_ref, margin_ref, own_ref, out_ref,
    raw, split, near, mine, rotated, theirs, diag, cross, packed, arrived,
    raw_sem, first_send, first_recv, block_send, block_recv, relay_send, proj_send, proj_recv, z_send, z_recv,
):
    kpt = lax.axis_index("kpt")
    band = lax.axis_index("band")
    other = 1 - band
    i = lax.div(kpt, SIZE_Y * SIZE_Z)
    j = lax.rem(lax.div(kpt, SIZE_Z), SIZE_Y)
    l = lax.rem(kpt, SIZE_Z)
    odd = lax.rem(l, 2)

    def point(di, dj, new_l):
        new_i = lax.rem(i + di + SIZE_X, SIZE_X)
        new_j = lax.rem(j + dj + SIZE_Y, SIZE_Y)
        return (new_i * SIZE_Y + new_j) * SIZE_Z + new_l

    l_near = l + 1 - 2 * odd
    l_far = lax.rem(l + 2 * odd - 1 + SIZE_Z, SIZE_Z)
    l_hop = lax.rem(l + 2 - 4 * odd + SIZE_Z, SIZE_Z)
    l_back = lax.rem(l - 2 + 4 * odd + SIZE_Z, SIZE_Z)

    steps = ((1, 0), (-1, 0), (0, 1), (0, -1))
    near_peers = [(point(-di, -dj, l_near), band) for di, dj in steps]
    far_peers = [(point(-di, -dj, l_far), other) for di, dj in steps]
    hop_peer = (point(0, 0, l_hop), other)
    back_peer = (point(0, 0, l_back), other)
    partner = (kpt, other)

    shell = [
        4 + odd, 6 + odd, 8 + odd, 10 + odd, 5 - odd, 7 - odd,
        0, 2, 1, 3, 9 - odd, 11 - odd,
    ]

    loads = [
        pltpu.make_async_copy(margin_ref.at[shell[s]], raw.at[s], raw_sem.at[s]) for s in range(SHELL)
    ]
    for load in loads:
        load.start()

    def clear(s, carry):
        near[s, ROWS:] = jnp.zeros((DEEP - ROWS, COLS), BF16)
        return carry

    lax.fori_loop(0, 2 * SHELL + 2, clear, 0)
    theirs[:, PAD:] = jnp.zeros((6, DEEP - PAD, COLS), BF16)

    barrier = pltpu.get_barrier_semaphore()
    peers = near_peers + far_peers[:2] + [hop_peer, back_peer, partner]
    for peer in peers:
        pl.semaphore_signal(barrier, inc=1, device_id=peer, device_id_type=MESH)
    pl.semaphore_wait(barrier, len(peers))

    def send(src, dst, send_sem, recv_sem, peer):
        copy = pltpu.make_async_remote_copy(
            src_ref=src, dst_ref=dst, send_sem=send_sem, recv_sem=recv_sem, device_id=peer, device_id_type=MESH
        )
        copy.start()
        return copy

    def block(s, q):
        return near.at[2 * s + q, pl.ds(0, ROWS)]

    def wait_block(s, q):
        pltpu.make_async_remote_copy(
            src_ref=block(s, q), dst_ref=block(s, q), send_sem=block_send.at[0, 0], recv_sem=block_recv.at[2 * s + q],
            device_id=partner, device_id_type=MESH,
        ).wait_recv()

    u_own = own_ref.at[0]
    u_other = near.at[2 * SHELL + 1, pl.ds(0, ROWS)]
    sent = []

    def direct(s, src, q, turn):
        peer = near_peers[s] if s < 4 else far_peers[s - 4]
        sent.append(send(src, block(s, q), block_send.at[s, turn], block_recv.at[2 * s + q], peer))

    first = send(u_own, u_other, first_send, first_recv, partner)
    for s in range(6):
        direct(s, u_own, band, 0)

    near[2 * SHELL, :ROWS] = own_ref[0]
    diag[...] = jnp.zeros_like(diag)
    cross[...] = jnp.zeros_like(cross)
    split[...] = jnp.zeros_like(split)
    for load in loads:
        load.wait()

    def separate(s, carry):
        whole = raw[s]
        for part in range(4):
            piece = whole[:, part * ROWS:(part + 1) * ROWS]
            split[2 * s + part % 2, (part // 2) * PAD:(part // 2) * PAD + ROWS, :ROWS] = piece
        return carry

    lax.fori_loop(0, 6, separate, 0)

    first.wait_recv()
    for s in range(6):
        direct(s, u_other, other, 1)

    lax.fori_loop(6, SHELL, separate, 0)

    def relays(s, q, turn):
        targets = {2: ((6, near_peers[0]), (7, near_peers[1]), (10, hop_peer)),
                   3: ((8, near_peers[0]), (9, near_peers[1]), (11, hop_peer))}[s]
        return [
            pltpu.make_async_remote_copy(
                src_ref=block(s, q), dst_ref=block(target, q), send_sem=relay_send.at[s, n, turn],
                recv_sem=block_recv.at[2 * target + q], device_id=peer, device_id_type=MESH,
            )
            for n, (target, peer) in enumerate(targets)
        ]

    def relay(s, q, turn):
        for copy in relays(s, q, turn):
            copy.start()

    row = lax.broadcasted_iota(jnp.int32, (PAD, 1), 0)
    inside = (row < ROWS) & (row + band * ROWS < window_ref[0])

    def project(s, carry):
        both = dot(split[2 * s], near[2 * s]) + dot(split[2 * s + 1], near[2 * s + 1])
        projected = jnp.where(inside, complex_rows(both, PAD, PAD), 0.0).astype(BF16)
        mine[s] = projected
        rotated[0:PAD] = projected
        rotated[PAD:, :HALF] = projected[:, HALF:]
        rotated[PAD:, HALF:] = -projected[:, :HALF]
        diag[...] += weight_ref[shell_of(s)] * dot_nt(rotated[...], projected)
        return carry

    def shell_of(s):
        near_b = 4 + 2 * s + odd
        far_x = 5 + 2 * (s - 4) - odd
        corner = 2 * lax.rem(s, 2) + lax.div(s - 6, 2)
        far_y = 9 + 2 * (s - 10) - odd
        return jnp.where(s < 4, near_b, jnp.where(s < 6, far_x, jnp.where(s < 10, corner, far_y)))

    def proj_copy(t):
        return pltpu.make_async_remote_copy(
            src_ref=mine.at[2 * t + band], dst_ref=theirs.at[t, pl.ds(0, PAD)],
            send_sem=proj_send.at[t], recv_sem=proj_recv.at[t], device_id=partner, device_id_type=MESH,
        )

    def meet(t):
        proj_copy(t).wait_recv()
        s = 2 * t + other
        projected = mine[s]
        rotated[0:PAD] = projected
        rotated[PAD:, :HALF] = projected[:, HALF:]
        rotated[PAD:, HALF:] = -projected[:, :HALF]
        cross[...] += weight_ref[shell_of(s)] * dot_nt(rotated[...], theirs[t])

    for s in (0, 1):
        wait_block(s, band)
    for s in (2, 3):
        wait_block(s, band)
        relay(s, band, 0)
    for s in (0, 1):
        wait_block(s, other)

    def pair(t, carry):
        @pl.when(t == 1)
        def _():
            for s in (2, 3):
                wait_block(s, other)
                relay(s, other, 1)

        @pl.when(t >= 2)
        def _():
            for u in range(2):
                for q in range(2):
                    wait_block(2 * t + u, q)

        lax.fori_loop(2 * t, 2 * t + 2, project, 0)
        proj_copy(t).start()

        @pl.when(t >= 1)
        def _():
            meet(t - 1)

        return carry

    lax.fori_loop(0, 6, pair, 0)
    meet(5)

    place_row = lax.broadcasted_iota(jnp.int32, (PAD, DEEP), 0)
    place_col = lax.broadcasted_iota(jnp.int32, (PAD, DEEP), 1)
    upper = place_row <= place_col
    packed[0] = cross[:PAD].astype(BF16)
    packed[1] = cross[PAD:].astype(BF16)
    packed[2, :, :PAD] = jnp.where(upper[:, :PAD], diag[:PAD], diag[PAD:]).astype(BF16)
    packed[2, :, PAD:] = jnp.zeros((PAD, DEEP - PAD), BF16)
    swap = send(packed, arrived, z_send, z_recv, partner)

    u_h = near[2 * SHELL]
    u_o = near[2 * SHELL + 1]
    diag_high, diag_low = halves(diag[...])
    cross_high, cross_low = halves(cross[...])
    x_h = (
        dot(diag_high, u_h[:PAD]) + dot(diag_low, u_h[:PAD]) + (dot(cross_high, u_o) + dot(cross_low, u_o))
    )
    flipped_high = jnp.concatenate([cross_high[:PAD], -cross_high[PAD:]], axis=1)
    flipped_low = jnp.concatenate([cross_low[:PAD], -cross_low[PAD:]], axis=1)
    x_o = dot_tn(flipped_high, u_h[:PAD]) + dot_tn(flipped_low, u_h[:PAD])

    swap.wait_recv()
    got = arrived[...]
    zero = jnp.zeros((PAD, DEEP), BF16)
    got_diag = got[2].astype(F32)
    got_real = jnp.where(upper, got_diag, 0.0).astype(BF16)
    got_above = jnp.where(place_row < place_col, got_diag, 0.0).astype(BF16)
    got_imag = jnp.where(upper, 0.0, got_diag).astype(BF16)
    x_h_late = dot_tn(jnp.concatenate([got[0], -got[1]], axis=1), u_o[:PAD])
    x_o_late = dot_tn(jnp.concatenate([got_above, -got_imag], axis=1), u_o[:PAD])
    x_o_plain = dot(jnp.concatenate([got_real, got_imag], axis=0), u_o) + dot(
        jnp.concatenate([got[0], got[1]], axis=0), u_h
    )
    x_h = complex_rows(x_h, PAD, PAD) + complex_rows(x_h_late, PAD, DEEP)
    x_o = complex_rows(x_o + x_o_late, PAD, DEEP) + complex_rows(x_o_plain, PAD, PAD)

    x_all = jnp.concatenate([x_h, x_o], axis=0)
    squares = jnp.sum(jnp.sum(x_all * x_all, axis=0, keepdims=True), axis=1, keepdims=True)
    scale = lax.rsqrt(2.0 * squares / HALF + 1e-06)
    gram = dot3(x_all, x_all, dot_tn) * (scale * scale)
    gram_real = gram[:HALF, :HALF] + gram[HALF:, HALF:]
    gram_imag = gram[:HALF, HALF:] - gram[HALF:, :HALF]
    eye = (
        lax.broadcasted_iota(jnp.int32, (HALF, HALF), 0) == lax.broadcasted_iota(jnp.int32, (HALF, HALF), 1)
    ).astype(F32)
    factor = stack_complex(1.5 * eye - 0.5 * gram_real, -0.5 * gram_imag)
    stacked = jnp.concatenate([x_h, jnp.concatenate([gram_real, gram_imag], axis=1)], axis=0)
    stacked = dot3(stacked, factor)
    gram = dot3(stacked[PAD:], factor)
    factor = stack_complex(1.5 * eye - 0.5 * gram[:, :HALF], -0.5 * gram[:, HALF:])
    out_ref[0] = (dot3(stacked[:PAD], factor) * (scale * math.sqrt(2.0 * ROWS)))[:ROWS]

    first.wait_send()
    for copy in sent:
        copy.wait_send()
    for s in (2, 3):
        for turn, q in enumerate((band, other)):
            for copy in relays(s, q, turn):
                copy.wait_send()
    for t in range(6):
        proj_copy(t).wait_send()
    swap.wait_send()


def on_device(margins, subspace, shell_weights, window_count):
    vmem = pl.BlockSpec(memory_space=pltpu.VMEM)
    smem = pl.BlockSpec(memory_space=pltpu.SMEM)
    return pl.pallas_call(
        kernel,
        out_shape=jax.ShapeDtypeStruct((1, ROWS, COLS), F32),
        in_specs=[smem, smem, pl.BlockSpec(memory_space=pl.ANY), vmem],
        out_specs=vmem,
        scratch_shapes=[
            pltpu.VMEM((SHELL, ROWS, 4 * ROWS), BF16),
            pltpu.VMEM((2 * SHELL, 2 * PAD, DEEP), BF16),
            pltpu.VMEM((2 * SHELL + 2, DEEP, COLS), BF16),
            pltpu.VMEM((SHELL, PAD, COLS), BF16),
            pltpu.VMEM((2 * PAD, COLS), BF16),
            pltpu.VMEM((6, DEEP, COLS), BF16),
            pltpu.VMEM((2 * PAD, PAD), F32),
            pltpu.VMEM((2 * PAD, DEEP), F32),
            pltpu.VMEM((3, PAD, DEEP), BF16),
            pltpu.VMEM((3, PAD, DEEP), BF16),
            pltpu.SemaphoreType.DMA((SHELL,)),
            pltpu.SemaphoreType.DMA,
            pltpu.SemaphoreType.DMA,
            pltpu.SemaphoreType.DMA((6, 2)),
            pltpu.SemaphoreType.DMA((2 * SHELL,)),
            pltpu.SemaphoreType.DMA((4, 3, 2)),
            pltpu.SemaphoreType.DMA((6,)),
            pltpu.SemaphoreType.DMA((6,)),
            pltpu.SemaphoreType.DMA,
            pltpu.SemaphoreType.DMA,
        ],
        compiler_params=pltpu.CompilerParams(
            collective_id=0, has_side_effects=True, vmem_limit_bytes=60 * 1024 * 1024
        ),
        name="disentangle",
    )(window_count, shell_weights, margins[0], subspace)


def solution(mesh):
    return jax.shard_map(
        on_device,
        mesh=mesh,
        in_specs=(P("kpt", None, "band", None), P("kpt", "band", None), P(), P("kpt")),
        out_specs=P("kpt", "band", None),
        check_vma=False,
    )
```

```python
import functools
import math

import jax
import jax.numpy as jnp
from jax import lax
from jax.experimental import pallas as pl
from jax.experimental.pallas import tpu as pltpu
from jax.sharding import PartitionSpec as P

SIZE_X, SIZE_Y, SIZE_Z = 4, 4, 8
ROWS = 200
PAD = 208
DEEP = 256
COLS = 512
HALF = 256
SHELL = 12
GIFTS = 3
MESH = pl.DeviceIdType.MESH
F32 = jnp.float32
BF16 = jnp.bfloat16

SHARED = 6
SLOTS = 9


def dot(a, b):
    return jnp.dot(a, b, preferred_element_type=F32)


def dot_nt(a, b):
    return lax.dot_general(a, b, (((1,), (1,)), ((), ())), preferred_element_type=F32)


def dot_tn(a, b):
    return lax.dot_general(a, b, (((0,), (0,)), ((), ())), preferred_element_type=F32)


def halves(a):
    high = a.astype(BF16)
    return high, (a - high.astype(F32)).astype(BF16)


def dot3(a, b, product=dot):
    a_high, a_low = halves(a)
    b_high, b_low = halves(b)
    return product(a_high, b_high) + (product(a_high, b_low) + product(a_low, b_high))


def complex_rows(both, rows, start):
    upper, lower = both[:rows], both[start:start + rows]
    return jnp.concatenate(
        [upper[:, :HALF] - lower[:, HALF:], upper[:, HALF:] + lower[:, :HALF]], axis=1
    )


def stack_complex(real, imag):
    return jnp.concatenate(
        [jnp.concatenate([real, imag], axis=1), jnp.concatenate([-imag, real], axis=1)], axis=0
    )


def unpacked_dots(block, upper, strict, subspace):
    block = block.astype(F32)
    real = jnp.where(upper, block, 0.0).astype(BF16)
    above = jnp.where(strict, block, 0.0).astype(BF16)
    imag = jnp.where(upper, 0.0, block).astype(BF16)
    plain = dot(jnp.concatenate([real, imag], axis=0), subspace)
    turned = dot_tn(jnp.concatenate([above, -imag], axis=1), subspace[:PAD])
    return plain, turned


def kernel(
    window_ref, weight_ref, margin_ref, own_ref, out_ref,
    raw, split, near, mine, alien, rotated, theirs, diag, other_diag, cross, packed, arrived,
    raw_sem, first_send, first_recv, gift_send, gift_recv, block_send, block_recv, relay_send,
    proj_send, proj_recv, z_send, z_recv,
):
    kpt = lax.axis_index("kpt")
    band = lax.axis_index("band")
    other = 1 - band
    i = lax.div(kpt, SIZE_Y * SIZE_Z)
    j = lax.rem(lax.div(kpt, SIZE_Z), SIZE_Y)
    l = lax.rem(kpt, SIZE_Z)
    odd = lax.rem(l, 2)
    minus = lax.rem(band + odd + lax.div(l, 2), 2)
    sign = 1 - 2 * minus

    def point(di, dj, new_l):
        new_i = lax.rem(i + di + SIZE_X, SIZE_X)
        new_j = lax.rem(j + dj + SIZE_Y, SIZE_Y)
        return (new_i * SIZE_Y + new_j) * SIZE_Z + new_l

    l_near = l + 1 - 2 * odd
    l_far = lax.rem(l + 2 * odd - 1 + SIZE_Z, SIZE_Z)
    l_hop = lax.rem(l + 2 - 4 * odd + SIZE_Z, SIZE_Z)
    l_back = lax.rem(l - 2 + 4 * odd + SIZE_Z, SIZE_Z)

    takers = [
        (point(sign, 0, l_near), band), (point(-sign, 0, l_near), band),
        (point(0, sign, l_near), band), (point(0, -sign, l_near), band),
        (point(sign, 0, l_far), other), (point(-sign, 0, l_far), other),
    ]
    hop_peer = (point(0, 0, l_hop), other)
    back_peer = (point(0, 0, l_back), other)
    partner = (kpt, other)

    plus = 1 - minus
    shell = [
        4 + 2 * minus + odd, 4 + 2 * plus + odd, 8 + 2 * minus + odd, 8 + 2 * plus + odd,
        5 + 2 * minus - odd, 5 + 2 * plus - odd, 1 + minus, 3 * plus, 9 + 2 * minus - odd,
    ]
    gift_shell = [1 + plus, 3 * minus, 9 + 2 * plus - odd]
    weights = [weight_ref[b] for b in shell]

    def weight_of(s):
        found = weights[0]
        for n in range(1, SLOTS):
            found = jnp.where(s == n, weights[n], found)
        return found

    loads = [
        pltpu.make_async_copy(margin_ref.at[shell[s]], raw.at[s], raw_sem.at[s]) for s in range(SLOTS)
    ]
    for load in loads:
        load.start()

    def clear(s, carry):
        near[s, ROWS:] = jnp.zeros((DEEP - ROWS, COLS), BF16)
        return carry

    lax.fori_loop(0, 2 * SLOTS + 2, clear, 0)
    theirs[:, PAD:] = jnp.zeros((3, DEEP - PAD, COLS), BF16)

    barrier = pltpu.get_barrier_semaphore()
    peers = takers + [hop_peer, back_peer, partner]
    for peer in peers:
        pl.semaphore_signal(barrier, inc=1, device_id=peer, device_id_type=MESH)
    pl.semaphore_wait(barrier, len(peers))

    def remote(src, dst, send_sem, recv_sem, peer):
        return pltpu.make_async_remote_copy(
            src_ref=src, dst_ref=dst, send_sem=send_sem, recv_sem=recv_sem, device_id=peer, device_id_type=MESH
        )

    def block(s, q):
        return near.at[2 * s + q, pl.ds(0, ROWS)]

    def wait_block(s, q):
        remote(block(s, q), block(s, q), block_send.at[0, 0], block_recv.at[2 * s + q], partner).wait_recv()

    u_own = own_ref.at[0]
    u_other = near.at[2 * SLOTS + 1, pl.ds(0, ROWS)]
    sent = []

    def direct(s, src, q, turn):
        copy = remote(src, block(s, q), block_send.at[s, turn], block_recv.at[2 * s + q], takers[s])
        copy.start()
        sent.append(copy)

    first = remote(u_own, u_other, first_send, first_recv, partner)
    first.start()
    for s in (2, 0, 1, 3, 4, 5):
        direct(s, u_own, band, 0)
    gifts = [
        remote(margin_ref.at[gift_shell[n]], raw.at[SLOTS + n], gift_send.at[n], gift_recv.at[n], partner)
        for n in range(GIFTS)
    ]
    for gift in gifts:
        gift.start()

    near[2 * SLOTS, :ROWS] = own_ref[0]
    diag[...] = jnp.zeros_like(diag)
    other_diag[...] = jnp.zeros_like(other_diag)
    cross[...] = jnp.zeros_like(cross)
    split[...] = jnp.zeros_like(split)
    for load in loads:
        load.wait()

    def separate(s, carry):
        whole = raw[s]
        for part in range(4):
            piece = whole[:, part * ROWS:(part + 1) * ROWS]
            split[2 * s + part % 2, (part // 2) * PAD:(part // 2) * PAD + ROWS, :ROWS] = piece
        return carry

    lax.fori_loop(0, 4, separate, 0)

    first.wait_recv()
    for s in (2, 0, 1, 3, 4, 5):
        direct(s, u_other, other, 1)

    def relays(q, turn):
        targets = ((6, takers[0]), (7, takers[1]), (8, hop_peer))
        return [
            remote(block(2, q), block(target, q), relay_send.at[n, turn], block_recv.at[2 * target + q], peer)
            for n, (target, peer) in enumerate(targets)
        ]

    wait_block(2, band)
    for copy in relays(band, 0):
        copy.start()
    lax.fori_loop(4, SLOTS, separate, 0)
    wait_block(2, other)
    for copy in relays(other, 1):
        copy.start()

    row = lax.broadcasted_iota(jnp.int32, (PAD, 1), 0)

    def projection(margin, s, owner):
        both = dot(split[2 * margin], near[2 * s]) + dot(split[2 * margin + 1], near[2 * s + 1])
        inside = (row < ROWS) & (row + owner * ROWS < window_ref[0])
        return jnp.where(inside, complex_rows(both, PAD, PAD), 0.0).astype(BF16)

    def turn_by(projected):
        rotated[0:PAD] = projected
        rotated[PAD:, :HALF] = projected[:, HALF:]
        rotated[PAD:, HALF:] = -projected[:, :HALF]

    def project(s, carry):
        projected = projection(s, s, band)
        mine[s] = projected
        turn_by(projected)
        diag[...] += weight_of(s) * dot_nt(rotated[...], projected)
        return carry

    def project_all(s, carry):
        aliens = projection(s + GIFTS, s, other)
        weight = weight_of(s)
        turn_by(aliens)
        other_diag[...] += weight * dot_nt(rotated[...], aliens)
        alien[0:PAD] = aliens
        projected = projection(s, s, band)
        turn_by(projected)
        diag[...] += weight * dot_nt(rotated[...], projected)
        cross[...] += weight * dot_nt(rotated[...], alien[...])
        return carry

    def proj_copy(t):
        return remote(
            mine.at[2 * t], theirs.at[t, pl.ds(0, PAD)], proj_send.at[t], proj_recv.at[t], partner
        )

    def meet(t):
        proj_copy(t).wait_recv()
        turn_by(mine[2 * t + 1])
        cross[...] += weight_of(2 * t + 1) * dot_nt(rotated[...], theirs[t])

    alien[PAD:] = jnp.zeros((DEEP - PAD, COLS), BF16)

    def pair(t, carry):
        for u in range(2):
            @pl.when((t != 1) | (u == 1))
            def _():
                for q in range(2):
                    wait_block(2 * t + u, q)

        lax.fori_loop(2 * t, 2 * t + 2, project, 0)
        proj_copy(t).start()
        return carry

    lax.fori_loop(0, SHARED // 2, pair, 0)

    def swapped(n, carry):
        remote(margin_ref.at[n], raw.at[SLOTS + n], gift_send.at[n], gift_recv.at[n], partner).wait_recv()
        separate(SLOTS + n, 0)
        for q in range(2):
            wait_block(SHARED + n, q)
        project_all(SHARED + n, 0)
        return carry

    lax.fori_loop(0, GIFTS, swapped, 0)

    place_row = lax.broadcasted_iota(jnp.int32, (PAD, DEEP), 0)
    place_col = lax.broadcasted_iota(jnp.int32, (PAD, DEEP), 1)
    upper = place_row <= place_col
    strict = place_row < place_col
    for n, ref in enumerate((diag, other_diag)):
        packed[n, :, :PAD] = jnp.where(upper[:, :PAD], ref[:PAD], ref[PAD:]).astype(BF16)
        packed[n, :, PAD:] = jnp.zeros((PAD, DEEP - PAD), BF16)
    swap = [
        remote(packed.at[pl.ds(2 * n, 2)], arrived.at[pl.ds(2 * n, 2)], z_send.at[n], z_recv.at[n], partner)
        for n in range(2)
    ]
    swap[0].start()

    def meet_all(t, carry):
        meet(t)
        return carry

    lax.fori_loop(0, SHARED // 2, meet_all, 0)
    packed[2] = cross[:PAD].astype(BF16)
    packed[3] = cross[PAD:].astype(BF16)
    swap[1].start()

    u_h = near[2 * SLOTS]
    u_o = near[2 * SLOTS + 1]
    diag_high, diag_low = halves(diag[...])
    alien_high, alien_low = halves(other_diag[...])
    cross_high, cross_low = halves(cross[...])
    x_h = dot(diag_high, u_h[:PAD]) + dot(diag_low, u_h[:PAD]) + (dot(cross_high, u_o) + dot(cross_low, u_o))
    x_o = dot(alien_high, u_o[:PAD]) + dot(alien_low, u_o[:PAD])
    flipped_high = jnp.concatenate([cross_high[:PAD], -cross_high[PAD:]], axis=1)
    flipped_low = jnp.concatenate([cross_low[:PAD], -cross_low[PAD:]], axis=1)
    x_o_turned = dot_tn(flipped_high, u_h[:PAD]) + dot_tn(flipped_low, u_h[:PAD])

    swap[0].wait_recv()
    plain, turned = unpacked_dots(arrived[0], upper, strict, u_o)
    x_o = x_o + plain
    x_o_turned = x_o_turned + turned
    plain, x_h_turned = unpacked_dots(arrived[1], upper, strict, u_h)
    x_h = x_h + plain

    swap[1].wait_recv()
    real, imag = arrived[2], arrived[3]
    x_h_turned = x_h_turned + dot_tn(jnp.concatenate([real, -imag], axis=1), u_o[:PAD])
    x_o = x_o + dot(jnp.concatenate([real, imag], axis=0), u_h)
    x_h = complex_rows(x_h, PAD, PAD) + complex_rows(x_h_turned, PAD, DEEP)
    x_o = complex_rows(x_o, PAD, PAD) + complex_rows(x_o_turned, PAD, DEEP)

    x_all = jnp.concatenate([x_h, x_o], axis=0)
    squares = jnp.sum(jnp.sum(x_all * x_all, axis=0, keepdims=True), axis=1, keepdims=True)
    scale = lax.rsqrt(2.0 * squares / HALF + 1e-06)
    gram = dot3(x_all, x_all, dot_tn) * (scale * scale)
    gram_real = gram[:HALF, :HALF] + gram[HALF:, HALF:]
    gram_imag = gram[:HALF, HALF:] - gram[HALF:, :HALF]
    eye = (
        lax.broadcasted_iota(jnp.int32, (HALF, HALF), 0) == lax.broadcasted_iota(jnp.int32, (HALF, HALF), 1)
    ).astype(F32)
    factor = stack_complex(1.5 * eye - 0.5 * gram_real, -0.5 * gram_imag)
    stacked = jnp.concatenate([x_h, jnp.concatenate([gram_real, gram_imag], axis=1)], axis=0)
    stacked = dot3(stacked, factor)
    gram = dot3(stacked[PAD:], factor)
    factor = stack_complex(1.5 * eye - 0.5 * gram[:, :HALF], -0.5 * gram[:, HALF:])
    out_ref[0] = (dot3(stacked[:PAD], factor) * (scale * math.sqrt(2.0 * ROWS)))[:ROWS]

    first.wait_send()
    for copy in sent + gifts + relays(band, 0) + relays(other, 1) + swap:
        copy.wait_send()
    for t in range(SHARED // 2):
        proj_copy(t).wait_send()


def on_device(margins, subspace, shell_weights, window_count):
    vmem = pl.BlockSpec(memory_space=pltpu.VMEM)
    smem = pl.BlockSpec(memory_space=pltpu.SMEM)
    return pl.pallas_call(
        kernel,
        out_shape=jax.ShapeDtypeStruct((1, ROWS, COLS), F32),
        in_specs=[smem, smem, pl.BlockSpec(memory_space=pl.ANY), vmem],
        out_specs=vmem,
        scratch_shapes=[
            pltpu.VMEM((SHELL, ROWS, 4 * ROWS), BF16),
            pltpu.VMEM((2 * SHELL, 2 * PAD, DEEP), BF16),
            pltpu.VMEM((2 * SLOTS + 2, DEEP, COLS), BF16),
            pltpu.VMEM((SHARED, PAD, COLS), BF16),
            pltpu.VMEM((DEEP, COLS), BF16),
            pltpu.VMEM((2 * PAD, COLS), BF16),
            pltpu.VMEM((SHARED // 2, DEEP, COLS), BF16),
            pltpu.VMEM((2 * PAD, PAD), F32),
            pltpu.VMEM((2 * PAD, PAD), F32),
            pltpu.VMEM((2 * PAD, DEEP), F32),
            pltpu.VMEM((4, PAD, DEEP), BF16),
            pltpu.VMEM((4, PAD, DEEP), BF16),
            pltpu.SemaphoreType.DMA((SLOTS,)),
            pltpu.SemaphoreType.DMA,
            pltpu.SemaphoreType.DMA,
            pltpu.SemaphoreType.DMA((GIFTS,)),
            pltpu.SemaphoreType.DMA((GIFTS,)),
            pltpu.SemaphoreType.DMA((6, 2)),
            pltpu.SemaphoreType.DMA((2 * SLOTS,)),
            pltpu.SemaphoreType.DMA((3, 2)),
            pltpu.SemaphoreType.DMA((SHARED // 2,)),
            pltpu.SemaphoreType.DMA((SHARED // 2,)),
            pltpu.SemaphoreType.DMA((2,)),
            pltpu.SemaphoreType.DMA((2,)),
        ],
        compiler_params=pltpu.CompilerParams(
            collective_id=0, has_side_effects=True, vmem_limit_bytes=60 * 1024 * 1024
        ),
        name="disentangle",
    )(window_count, shell_weights, margins[0], subspace)


def solution(mesh):
    return jax.shard_map(
        on_device,
        mesh=mesh,
        in_specs=(P("kpt", None, "band", None), P("kpt", "band", None), P(), P("kpt")),
        out_specs=P("kpt", "band", None),
        check_vma=False,
    )
```

```python
import functools
import math

import jax
import jax.numpy as jnp
from jax import lax
from jax.experimental import pallas as pl
from jax.experimental.pallas import tpu as pltpu
from jax.sharding import PartitionSpec as P

SIZE_X, SIZE_Y, SIZE_Z = 4, 4, 8
ROWS = 200
PAD = 208
DEEP = 256
COLS = 512
HALF = 256
SHELL = 12
GIFTS = 4
STEM = 768
TAIL = 4 * ROWS - STEM
WIDE = 384
REST = 2 * ROWS - WIDE
MESH = pl.DeviceIdType.MESH
F32 = jnp.float32
BF16 = jnp.bfloat16

SHARED = 4
SLOTS = 8
FAR = SLOTS + 1


def dot(a, b):
    return jnp.dot(a, b, preferred_element_type=F32)


def dot_nt(a, b):
    return lax.dot_general(a, b, (((1,), (1,)), ((), ())), preferred_element_type=F32)


def dot_tn(a, b):
    return lax.dot_general(a, b, (((0,), (0,)), ((), ())), preferred_element_type=F32)


def halves(a):
    high = a.astype(BF16)
    return high, (a - high.astype(F32)).astype(BF16)


def dot3(a, b, product=dot):
    a_high, a_low = halves(a)
    b_high, b_low = halves(b)
    return product(a_high, b_high) + (product(a_high, b_low) + product(a_low, b_high))


def complex_rows(both, rows, start):
    upper, lower = both[:rows], both[start:start + rows]
    return jnp.concatenate(
        [upper[:, :HALF] - lower[:, HALF:], upper[:, HALF:] + lower[:, :HALF]], axis=1
    )


def stack_complex(real, imag):
    return jnp.concatenate(
        [jnp.concatenate([real, imag], axis=1), jnp.concatenate([-imag, real], axis=1)], axis=0
    )


def unpacked_dots(block, upper, strict, subspace):
    block = block.astype(F32)
    real = jnp.where(upper, block, 0.0).astype(BF16)
    above = jnp.where(strict, block, 0.0).astype(BF16)
    imag = jnp.where(upper, 0.0, block).astype(BF16)
    plain = dot(jnp.concatenate([real, imag], axis=0), subspace)
    turned = dot_tn(jnp.concatenate([above, -imag], axis=1), subspace[:PAD])
    return plain, turned


def kernel(
    window_ref, weight_ref, margin_ref, own_ref, out_ref,
    raw, spare, tails, given, split, near, mine, alien, rotated, theirs, diag, other_diag, cross, packed, arrived,
    own_sem, raw_sem, first_send, first_recv, gift_send, gift_recv, block_send, block_recv,
    proj_send, proj_recv, z_send, z_recv,
):
    kpt = lax.axis_index("kpt")
    band = lax.axis_index("band")
    other = 1 - band
    i = lax.div(kpt, SIZE_Y * SIZE_Z)
    j = lax.rem(lax.div(kpt, SIZE_Z), SIZE_Y)
    l = lax.rem(kpt, SIZE_Z)
    odd = lax.rem(l, 2)
    minus = lax.rem(band + odd + lax.div(l, 2), 2)
    sign = 1 - 2 * minus

    def point(di, dj, new_l):
        new_i = lax.rem(i + di + SIZE_X, SIZE_X)
        new_j = lax.rem(j + dj + SIZE_Y, SIZE_Y)
        return (new_i * SIZE_Y + new_j) * SIZE_Z + new_l

    l_near = l + 1 - 2 * odd
    l_far = lax.rem(l + 2 * odd - 1 + SIZE_Z, SIZE_Z)
    l_hop = lax.rem(l + 2 - 4 * odd + SIZE_Z, SIZE_Z)
    l_back = lax.rem(l - 2 + 4 * odd + SIZE_Z, SIZE_Z)

    takers = [
        (point(sign, 0, l_near), band), (point(-sign, 0, l_near), band),
        (point(0, sign, l_near), band),
    ]
    far_peer = (point(0, 0, l_far), other)
    far_takers = [(point(-sign, 0, l), band), (point(sign, 0, l), band)]
    hop_peer = (point(0, 0, l_hop), other)
    back_peer = (point(0, 0, l_back), other)
    partner = (kpt, other)

    plus = 1 - minus
    shell = [
        4 + 2 * minus + odd, 4 + 2 * plus + odd, 5 + 2 * minus - odd, 5 + 2 * plus - odd,
        8 + 2 * minus + odd, 1 + minus, 3 * plus, 9 + 2 * minus - odd,
    ]
    gift_shell = [8 + 2 * plus + odd, 1 + plus, 3 * minus, 9 + 2 * plus - odd]
    weights = [weight_ref[b] for b in shell]

    def weight_of(s):
        found = weights[0]
        for n in range(1, SLOTS):
            found = jnp.where(s == n, weights[n], found)
        return found

    loads = [
        pltpu.make_async_copy(margin_ref.at[shell[s]], raw.at[s], raw_sem.at[s]) for s in range(SLOTS)
    ]
    u_own = near.at[2 * SLOTS, pl.ds(0, ROWS)]
    own_load = pltpu.make_async_copy(own_ref.at[0], u_own, own_sem)
    own_load.start()
    gift_loads = [
        pltpu.make_async_copy(margin_ref.at[gift_shell[n]], spare.at[n], raw_sem.at[SLOTS + n]) for n in range(GIFTS)
    ]
    for load in loads + gift_loads:
        load.start()

    def clear(s, carry):
        near[s, ROWS:] = jnp.zeros((DEEP - ROWS, COLS), BF16)
        return carry

    lax.fori_loop(0, 2 * SLOTS + 2, clear, 0)
    theirs[:, ROWS:] = jnp.zeros((SHARED // 2, DEEP - ROWS, COLS), BF16)

    barrier = pltpu.get_barrier_semaphore()
    peers = takers + far_takers + [far_peer, hop_peer, back_peer, partner]
    for peer in peers:
        pl.semaphore_signal(barrier, inc=1, device_id=peer, device_id_type=MESH)
    pl.semaphore_wait(barrier, len(peers))

    def remote(src, dst, send_sem, recv_sem, peer):
        return pltpu.make_async_remote_copy(
            src_ref=src, dst_ref=dst, send_sem=send_sem, recv_sem=recv_sem, device_id=peer, device_id_type=MESH
        )

    def block(s, q):
        return near.at[2 * s + q, pl.ds(0, ROWS)]

    def wait_block(s, q):
        remote(block(s, q), block(s, q), block_send.at[0], block_recv.at[2 * s + q], partner).wait_recv()

    u_other = near.at[2 * SLOTS + 1, pl.ds(0, ROWS)]
    sent = []

    def pass_on(src, s, q, turn, peer):
        copy = remote(src, block(s, q), block_send.at[2 * s + turn], block_recv.at[2 * s + q], peer)
        copy.start()
        sent.append(copy)

    first = remote(u_own, u_other, first_send, first_recv, partner)
    own_load.wait()
    first.start()
    def offer(src, q, turn):
        pass_on(src, 4, q, turn, takers[2])
        pass_on(src, FAR, q, turn, far_peer)
        for s in (0, 1):
            pass_on(src, s, q, turn, takers[s])

    offer(u_own, band, 0)
    gifts = [
        remote(
            margin_ref.at[gift_shell[n], :, pl.ds(0, STEM)], raw.at[SLOTS + n, :, pl.ds(0, STEM)], gift_send.at[n],
            gift_recv.at[n], partner,
        )
        for n in range(GIFTS)
    ]
    tail_gift = remote(tails, given, gift_send.at[GIFTS], gift_recv.at[GIFTS], partner)
    for gift in gifts:
        gift.start()

    diag[...] = jnp.zeros_like(diag)
    other_diag[...] = jnp.zeros_like(other_diag)
    cross[...] = jnp.zeros_like(cross)
    split[...] = jnp.zeros_like(split)
    for load in loads + gift_loads:
        load.wait()
    for n in range(GIFTS):
        tails[:, n * TAIL:(n + 1) * TAIL] = spare[n, :, STEM:]

    def separate(s, carry):
        whole = raw[s]
        for part in range(4):
            piece = whole[:, part * ROWS:(part + 1) * ROWS]
            split[2 * s + part % 2, (part // 2) * PAD:(part // 2) * PAD + ROWS, :ROWS] = piece
        return carry

    lax.fori_loop(0, 4, separate, 0)
    tail_gift.start()

    first.wait_recv()
    offer(u_other, other, 1)

    for turn, q in enumerate((band, other)):
        wait_block(FAR, q)
        for n in range(2):
            pass_on(block(FAR, q), 2 + n, q, turn, far_takers[n])
        wait_block(4, q)
        for n in range(2):
            pass_on(block(4, q), 5 + n, q, turn, takers[n])
        pass_on(block(4, q), 7, q, turn, hop_peer)
        if turn == 0:
            lax.fori_loop(4, SLOTS, separate, 0)

    row = lax.broadcasted_iota(jnp.int32, (PAD, 1), 0)

    def projection(margin, s, owner):
        both = dot(split[2 * margin], near[2 * s]) + dot(split[2 * margin + 1], near[2 * s + 1])
        inside = (row < ROWS) & (row + owner * ROWS < window_ref[0])
        return jnp.where(inside, complex_rows(both, PAD, PAD), 0.0).astype(BF16)

    def turn_by(projected):
        rotated[0:PAD] = projected
        rotated[PAD:, :HALF] = projected[:, HALF:]
        rotated[PAD:, HALF:] = -projected[:, :HALF]

    def project(s, carry):
        projected = projection(s, s, band)
        mine[s] = projected
        turn_by(projected)
        diag[...] += weight_of(s) * dot_nt(rotated[...], projected)
        return carry

    def project_all(s, carry):
        aliens = projection(s + GIFTS, s, other)
        weight = weight_of(s)
        turn_by(aliens)
        other_diag[...] += weight * dot_nt(rotated[...], aliens)
        alien[0:PAD] = aliens
        projected = projection(s, s, band)
        turn_by(projected)
        diag[...] += weight * dot_nt(rotated[...], projected)
        cross[...] += weight * dot_nt(rotated[...], alien[...])
        return carry

    def proj_copy(t):
        return remote(
            mine.at[2 * t, pl.ds(0, ROWS)], theirs.at[t, pl.ds(0, ROWS)], proj_send.at[t], proj_recv.at[t], partner
        )

    def meet(t):
        proj_copy(t).wait_recv()
        turn_by(mine[2 * t + 1])
        cross[...] += weight_of(2 * t + 1) * dot_nt(rotated[...], theirs[t])

    alien[PAD:] = jnp.zeros((DEEP - PAD, COLS), BF16)

    def pair(t, carry):
        lax.fori_loop(2 * t, 2 * t + 2, project, 0)
        proj_copy(t).start()
        return carry

    def wait_pair(t, carry):
        for u in range(2):
            for q in range(2):
                wait_block(2 * t + u, q)
        return carry

    def shared(t, carry):
        wait_pair(t, 0)
        return pair(t, carry)

    def swapped(n, carry):
        separate(SLOTS + n, 0)

        @pl.when(n > 0)
        def _():
            for q in range(2):
                wait_block(SHARED + n, q)

        project_all(SHARED + n, 0)
        return carry

    lax.fori_loop(0, SHARED // 2, shared, 0)
    tail_gift.wait_recv()
    for n in range(GIFTS):
        gifts[n].wait_recv()
        raw[SLOTS + n, :, STEM:] = given[:, n * TAIL:(n + 1) * TAIL]
    lax.fori_loop(0, GIFTS, swapped, 0)

    place_row = lax.broadcasted_iota(jnp.int32, (PAD, DEEP), 0)
    place_col = lax.broadcasted_iota(jnp.int32, (PAD, DEEP), 1)
    upper = place_row <= place_col
    strict = place_row < place_col
    pick = (
        lax.broadcasted_iota(jnp.int32, (REST, DEEP), 1) == ROWS - REST + lax.broadcasted_iota(jnp.int32, (REST, DEEP), 0)
    ).astype(BF16)

    def pack(n, left, right):
        left, right = left.astype(BF16), right.astype(BF16)
        packed[n, :PAD] = jnp.concatenate([left[:, :ROWS], right[:, :ROWS - REST]], axis=1)
        packed[n, PAD:, :PAD] = dot_nt(pick[:, :PAD], right).astype(BF16)

    def unpack(n):
        both = arrived[n, :PAD]
        left = jnp.where(place_col < ROWS, both[:, :DEEP].astype(F32), 0.0).astype(BF16)
        shifted = jnp.concatenate([both[:, ROWS:], jnp.zeros((PAD, DEEP - WIDE + ROWS), BF16)], axis=1)
        rest = dot_tn(arrived[n, PAD:, :PAD], pick)
        return left, (shifted.astype(F32) + rest).astype(BF16)

    packed[:, PAD:] = jnp.zeros((2, REST, WIDE), BF16)
    square = upper[:, :PAD]
    pack(0, jnp.where(square, diag[:PAD], diag[PAD:]), jnp.where(square, other_diag[:PAD], other_diag[PAD:]))
    swap = [remote(packed.at[n], arrived.at[n], z_send.at[n], z_recv.at[n], partner) for n in range(2)]
    swap[0].start()

    def meet_all(t, carry):
        meet(t)
        return carry

    lax.fori_loop(0, SHARED // 2, meet_all, 0)
    pack(1, cross[:PAD, :PAD], cross[PAD:, :PAD])
    swap[1].start()

    u_h = near[2 * SLOTS]
    u_o = near[2 * SLOTS + 1]
    diag_high, diag_low = halves(diag[...])
    alien_high, alien_low = halves(other_diag[...])
    cross_high, cross_low = halves(cross[...])
    x_h = dot(diag_high, u_h[:PAD]) + dot(diag_low, u_h[:PAD]) + (dot(cross_high, u_o) + dot(cross_low, u_o))
    x_o = dot(alien_high, u_o[:PAD]) + dot(alien_low, u_o[:PAD])
    flipped_high = jnp.concatenate([cross_high[:PAD], -cross_high[PAD:]], axis=1)
    flipped_low = jnp.concatenate([cross_low[:PAD], -cross_low[PAD:]], axis=1)
    x_o_turned = dot_tn(flipped_high, u_h[:PAD]) + dot_tn(flipped_low, u_h[:PAD])

    swap[0].wait_recv()
    theirs_own, theirs_other = unpack(0)
    plain, turned = unpacked_dots(theirs_own, upper, strict, u_o)
    x_o = x_o + plain
    x_o_turned = x_o_turned + turned
    plain, x_h_turned = unpacked_dots(theirs_other, upper, strict, u_h)
    x_h = x_h + plain

    swap[1].wait_recv()
    real, imag = unpack(1)
    x_h_turned = x_h_turned + dot_tn(jnp.concatenate([real, -imag], axis=1), u_o[:PAD])
    x_o = x_o + dot(jnp.concatenate([real, imag], axis=0), u_h)
    x_h = complex_rows(x_h, PAD, PAD) + complex_rows(x_h_turned, PAD, DEEP)
    x_o = complex_rows(x_o, PAD, PAD) + complex_rows(x_o_turned, PAD, DEEP)

    x_all = jnp.concatenate([x_h, x_o], axis=0)
    squares = jnp.sum(jnp.sum(x_all * x_all, axis=0, keepdims=True), axis=1, keepdims=True)
    scale = lax.rsqrt(2.0 * squares / HALF + 1e-06)
    gram = dot3(x_all, x_all, dot_tn) * (scale * scale)
    gram_real = gram[:HALF, :HALF] + gram[HALF:, HALF:]
    gram_imag = gram[:HALF, HALF:] - gram[HALF:, :HALF]
    eye = (
        lax.broadcasted_iota(jnp.int32, (HALF, HALF), 0) == lax.broadcasted_iota(jnp.int32, (HALF, HALF), 1)
    ).astype(F32)
    factor = stack_complex(1.5 * eye - 0.5 * gram_real, -0.5 * gram_imag)
    stacked = jnp.concatenate([x_h, jnp.concatenate([gram_real, gram_imag], axis=1)], axis=0)
    stacked = dot3(stacked, factor)
    gram = dot3(stacked[PAD:], factor)
    factor = stack_complex(1.5 * eye - 0.5 * gram[:, :HALF], -0.5 * gram[:, HALF:])
    out_ref[0] = (dot3(stacked[:PAD], factor) * (scale * math.sqrt(2.0 * ROWS)))[:ROWS]

    first.wait_send()
    for copy in sent + gifts + [tail_gift] + swap:
        copy.wait_send()
    for t in range(SHARED // 2):
        proj_copy(t).wait_send()


def on_device(margins, subspace, shell_weights, window_count):
    vmem = pl.BlockSpec(memory_space=pltpu.VMEM)
    smem = pl.BlockSpec(memory_space=pltpu.SMEM)
    return pl.pallas_call(
        kernel,
        out_shape=jax.ShapeDtypeStruct((1, ROWS, COLS), F32),
        in_specs=[smem, smem, pl.BlockSpec(memory_space=pl.ANY), pl.BlockSpec(memory_space=pl.ANY)],
        out_specs=vmem,
        scratch_shapes=[
            pltpu.VMEM((SHELL, ROWS, 4 * ROWS), BF16),
            pltpu.VMEM((GIFTS, ROWS, 4 * ROWS), BF16),
            pltpu.VMEM((ROWS, GIFTS * TAIL), BF16),
            pltpu.VMEM((ROWS, GIFTS * TAIL), BF16),
            pltpu.VMEM((2 * SHELL, 2 * PAD, DEEP), BF16),
            pltpu.VMEM((2 * SLOTS + 4, DEEP, COLS), BF16),
            pltpu.VMEM((SHARED, PAD, COLS), BF16),
            pltpu.VMEM((DEEP, COLS), BF16),
            pltpu.VMEM((2 * PAD, COLS), BF16),
            pltpu.VMEM((SHARED // 2, DEEP, COLS), BF16),
            pltpu.VMEM((2 * PAD, PAD), F32),
            pltpu.VMEM((2 * PAD, PAD), F32),
            pltpu.VMEM((2 * PAD, DEEP), F32),
            pltpu.VMEM((2, PAD + REST, WIDE), BF16),
            pltpu.VMEM((2, PAD + REST, WIDE), BF16),
            pltpu.SemaphoreType.DMA,
            pltpu.SemaphoreType.DMA((SLOTS + GIFTS,)),
            pltpu.SemaphoreType.DMA,
            pltpu.SemaphoreType.DMA,
            pltpu.SemaphoreType.DMA((GIFTS + 1,)),
            pltpu.SemaphoreType.DMA((GIFTS + 1,)),
            pltpu.SemaphoreType.DMA((2 * FAR + 2,)),
            pltpu.SemaphoreType.DMA((2 * FAR + 2,)),
            pltpu.SemaphoreType.DMA((SHARED // 2,)),
            pltpu.SemaphoreType.DMA((SHARED // 2,)),
            pltpu.SemaphoreType.DMA((2,)),
            pltpu.SemaphoreType.DMA((2,)),
        ],
        compiler_params=pltpu.CompilerParams(
            collective_id=0, has_side_effects=True, vmem_limit_bytes=60 * 1024 * 1024
        ),
        name="disentangle",
    )(window_count, shell_weights, margins[0], subspace)


def solution(mesh):
    return jax.shard_map(
        on_device,
        mesh=mesh,
        in_specs=(P("kpt", None, "band", None), P("kpt", "band", None), P(), P("kpt")),
        out_specs=P("kpt", "band", None),
        check_vma=False,
    )
```

```python
import functools
import math

import jax
import jax.numpy as jnp
from jax import lax
from jax.experimental import pallas as pl
from jax.experimental.pallas import tpu as pltpu
from jax.sharding import PartitionSpec as P

SIZE_X, SIZE_Y, SIZE_Z = 4, 4, 8
ROWS = 200
PAD = 208
DEEP = 256
COLS = 512
HALF = 256
SHELL = 12
GIFTS = 4
STEM = 768
TAIL = 4 * ROWS - STEM
WIDE = 384
REST = 2 * ROWS - WIDE
MESH = pl.DeviceIdType.MESH
F32 = jnp.float32
BF16 = jnp.bfloat16

SHARED = 4
SLOTS = 8
FAR = SLOTS + 1


def dot(a, b):
    return jnp.dot(a, b, preferred_element_type=F32)


def dot_nt(a, b):
    return lax.dot_general(a, b, (((1,), (1,)), ((), ())), preferred_element_type=F32)


def dot_tn(a, b):
    return lax.dot_general(a, b, (((0,), (0,)), ((), ())), preferred_element_type=F32)


def halves(a):
    high = a.astype(BF16)
    return high, (a - high.astype(F32)).astype(BF16)


def dot3(a, b, product=dot):
    a_high, a_low = halves(a)
    b_high, b_low = halves(b)
    return product(a_high, b_high) + (product(a_high, b_low) + product(a_low, b_high))


def complex_rows(both, rows, start):
    upper, lower = both[:rows], both[start:start + rows]
    return jnp.concatenate(
        [upper[:, :HALF] - lower[:, HALF:], upper[:, HALF:] + lower[:, :HALF]], axis=1
    )


def stack_complex(real, imag):
    return jnp.concatenate(
        [jnp.concatenate([real, imag], axis=1), jnp.concatenate([-imag, real], axis=1)], axis=0
    )


def unpacked_dots(block, upper, strict, subspace):
    block = block.astype(F32)
    real = jnp.where(upper, block, 0.0).astype(BF16)
    above = jnp.where(strict, block, 0.0).astype(BF16)
    imag = jnp.where(upper, 0.0, block).astype(BF16)
    plain = dot(jnp.concatenate([real, imag], axis=0), subspace)
    turned = dot_tn(jnp.concatenate([above, -imag], axis=1), subspace[:PAD])
    return plain, turned


def kernel(
    window_ref, weight_ref, margin_ref, own_ref, out_ref,
    raw, spare, tails, given, split, near, mine, alien, rotated, theirs, diag, other_diag, cross, packed, arrived,
    own_sem, raw_sem, first_send, first_recv, gift_send, gift_recv, block_send, block_recv,
    proj_send, proj_recv, z_send, z_recv,
):
    kpt = lax.axis_index("kpt")
    band = lax.axis_index("band")
    other = 1 - band
    i = lax.div(kpt, SIZE_Y * SIZE_Z)
    j = lax.rem(lax.div(kpt, SIZE_Z), SIZE_Y)
    l = lax.rem(kpt, SIZE_Z)
    odd = lax.rem(l, 2)
    minus = lax.rem(band + odd + lax.div(l, 2), 2)
    sign = 1 - 2 * minus

    def point(di, dj, new_l):
        new_i = lax.rem(i + di + SIZE_X, SIZE_X)
        new_j = lax.rem(j + dj + SIZE_Y, SIZE_Y)
        return (new_i * SIZE_Y + new_j) * SIZE_Z + new_l

    l_near = l + 1 - 2 * odd
    l_far = lax.rem(l + 2 * odd - 1 + SIZE_Z, SIZE_Z)
    l_hop = lax.rem(l + 2 - 4 * odd + SIZE_Z, SIZE_Z)
    l_back = lax.rem(l - 2 + 4 * odd + SIZE_Z, SIZE_Z)

    takers = [
        (point(sign, 0, l_near), band), (point(-sign, 0, l_near), band),
        (point(0, sign, l_near), band),
    ]
    far_peer = (point(0, 0, l_far), other)
    far_takers = [(point(-sign, 0, l), band), (point(sign, 0, l), band)]
    hop_peer = (point(0, 0, l_hop), other)
    back_peer = (point(0, 0, l_back), other)
    partner = (kpt, other)

    plus = 1 - minus
    shell = [
        4 + 2 * minus + odd, 4 + 2 * plus + odd, 5 + 2 * minus - odd, 5 + 2 * plus - odd,
        8 + 2 * minus + odd, 1 + minus, 3 * plus, 9 + 2 * minus - odd,
    ]
    gift_shell = [8 + 2 * plus + odd, 1 + plus, 3 * minus, 9 + 2 * plus - odd]
    weights = [weight_ref[b] for b in shell]

    def weight_of(s):
        found = weights[0]
        for n in range(1, SLOTS):
            found = jnp.where(s == n, weights[n], found)
        return found

    loads = [
        pltpu.make_async_copy(margin_ref.at[shell[s]], raw.at[s], raw_sem.at[s]) for s in range(SLOTS)
    ]
    u_own = near.at[2 * SLOTS, pl.ds(0, ROWS)]
    own_load = pltpu.make_async_copy(own_ref.at[0], u_own, own_sem)
    own_load.start()
    gift_loads = [
        pltpu.make_async_copy(margin_ref.at[gift_shell[n]], spare.at[n], raw_sem.at[SLOTS + n]) for n in range(GIFTS)
    ]
    for load in loads + gift_loads:
        load.start()

    def clear(s, carry):
        near[s, ROWS:] = jnp.zeros((DEEP - ROWS, COLS), BF16)
        return carry

    lax.fori_loop(0, 2 * SLOTS + 2, clear, 0)
    theirs[:, ROWS:] = jnp.zeros((SHARED // 2, DEEP - ROWS, COLS), BF16)

    barrier = pltpu.get_barrier_semaphore()
    peers = takers + far_takers + [far_peer, hop_peer, back_peer, partner]
    for peer in peers:
        pl.semaphore_signal(barrier, inc=1, device_id=peer, device_id_type=MESH)
    pl.semaphore_wait(barrier, len(peers))

    def remote(src, dst, send_sem, recv_sem, peer):
        return pltpu.make_async_remote_copy(
            src_ref=src, dst_ref=dst, send_sem=send_sem, recv_sem=recv_sem, device_id=peer, device_id_type=MESH
        )

    def block(s, q):
        return near.at[2 * s + q, pl.ds(0, ROWS)]

    def wait_block(s, q):
        remote(block(s, q), block(s, q), block_send.at[0], block_recv.at[2 * s + q], partner).wait_recv()

    u_other = near.at[2 * SLOTS + 1, pl.ds(0, ROWS)]
    sent = []

    def pass_on(src, s, q, turn, peer):
        copy = remote(src, block(s, q), block_send.at[2 * s + turn], block_recv.at[2 * s + q], peer)
        copy.start()
        sent.append(copy)

    first = remote(u_own, u_other, first_send, first_recv, partner)
    own_load.wait()
    first.start()
    def offer(src, q, turn):
        pass_on(src, 4, q, turn, takers[2])
        pass_on(src, FAR, q, turn, far_peer)
        for s in (0, 1):
            pass_on(src, s, q, turn, takers[s])

    offer(u_own, band, 0)
    gifts = [
        remote(
            margin_ref.at[gift_shell[n], :, pl.ds(0, STEM)], raw.at[SLOTS + n, :, pl.ds(0, STEM)], gift_send.at[n],
            gift_recv.at[n], partner,
        )
        for n in range(GIFTS)
    ]
    tail_gift = remote(tails, given, gift_send.at[GIFTS], gift_recv.at[GIFTS], partner)

    diag[...] = jnp.zeros_like(diag)
    other_diag[...] = jnp.zeros_like(other_diag)
    cross[...] = jnp.zeros_like(cross)
    split[...] = jnp.zeros_like(split)
    for load in loads + gift_loads:
        load.wait()
    for n in range(GIFTS):
        tails[:, n * TAIL:(n + 1) * TAIL] = spare[n, :, STEM:]

    def separate(s, carry):
        whole = raw[s]
        for part in range(4):
            piece = whole[:, part * ROWS:(part + 1) * ROWS]
            split[2 * s + part % 2, (part // 2) * PAD:(part // 2) * PAD + ROWS, :ROWS] = piece
        return carry

    gifts[0].start()
    lax.fori_loop(0, 4, separate, 0)
    tail_gift.start()
    for gift in gifts[1:]:
        gift.start()

    first.wait_recv()
    offer(u_other, other, 1)

    for turn, q in enumerate((band, other)):
        wait_block(FAR, q)
        for n in range(2):
            pass_on(block(FAR, q), 2 + n, q, turn, far_takers[n])
        wait_block(4, q)
        for n in range(2):
            pass_on(block(4, q), 5 + n, q, turn, takers[n])
        pass_on(block(4, q), 7, q, turn, hop_peer)
        if turn == 0:
            lax.fori_loop(4, SLOTS, separate, 0)

    row = lax.broadcasted_iota(jnp.int32, (PAD, 1), 0)

    def projection(margin, s, owner):
        both = dot(split[2 * margin], near[2 * s]) + dot(split[2 * margin + 1], near[2 * s + 1])
        inside = (row < ROWS) & (row + owner * ROWS < window_ref[0])
        return jnp.where(inside, complex_rows(both, PAD, PAD), 0.0).astype(BF16)

    def turn_by(projected):
        rotated[0:PAD] = projected
        rotated[PAD:, :HALF] = projected[:, HALF:]
        rotated[PAD:, HALF:] = -projected[:, :HALF]

    def project(s, carry):
        projected = projection(s, s, band)
        mine[s] = projected
        turn_by(projected)
        diag[...] += weight_of(s) * dot_nt(rotated[...], projected)
        return carry

    def project_all(s, carry):
        aliens = projection(s + GIFTS, s, other)
        weight = weight_of(s)
        turn_by(aliens)
        other_diag[...] += weight * dot_nt(rotated[...], aliens)
        alien[0:PAD] = aliens
        projected = projection(s, s, band)
        turn_by(projected)
        diag[...] += weight * dot_nt(rotated[...], projected)
        cross[...] += weight * dot_nt(rotated[...], alien[...])
        return carry

    def proj_copy(t):
        return remote(
            mine.at[2 * t, pl.ds(0, ROWS)], theirs.at[t, pl.ds(0, ROWS)], proj_send.at[t], proj_recv.at[t], partner
        )

    def meet(t):
        proj_copy(t).wait_recv()
        turn_by(mine[2 * t + 1])
        cross[...] += weight_of(2 * t + 1) * dot_nt(rotated[...], theirs[t])

    alien[PAD:] = jnp.zeros((DEEP - PAD, COLS), BF16)

    def pair(t, carry):
        lax.fori_loop(2 * t, 2 * t + 2, project, 0)
        proj_copy(t).start()
        return carry

    def wait_pair(t, carry):
        for u in range(2):
            for q in range(2):
                wait_block(2 * t + u, q)
        return carry

    def shared(t, carry):
        wait_pair(t, 0)
        return pair(t, carry)

    def swapped(n, carry):
        stem = raw.at[SLOTS + n, :, pl.ds(0, STEM)]
        remote(stem, stem, gift_send.at[n], gift_recv.at[n], partner).wait_recv()
        separate(SLOTS + n, 0)

        @pl.when(n > 0)
        def _():
            for q in range(2):
                wait_block(SHARED + n, q)

        project_all(SHARED + n, 0)
        return carry

    lax.fori_loop(0, SHARED // 2, shared, 0)
    tail_gift.wait_recv()
    for n in range(GIFTS):
        raw[SLOTS + n, :, STEM:] = given[:, n * TAIL:(n + 1) * TAIL]
    lax.fori_loop(0, GIFTS, swapped, 0)

    place_row = lax.broadcasted_iota(jnp.int32, (PAD, DEEP), 0)
    place_col = lax.broadcasted_iota(jnp.int32, (PAD, DEEP), 1)
    upper = place_row <= place_col
    strict = place_row < place_col
    pick = (
        lax.broadcasted_iota(jnp.int32, (REST, DEEP), 1) == ROWS - REST + lax.broadcasted_iota(jnp.int32, (REST, DEEP), 0)
    ).astype(BF16)

    def pack(n, left, right):
        left, right = left.astype(BF16), right.astype(BF16)
        packed[n, :PAD] = jnp.concatenate([left[:, :ROWS], right[:, :ROWS - REST]], axis=1)
        packed[n, PAD:, :PAD] = dot_nt(pick[:, :PAD], right).astype(BF16)

    def unpack(n):
        both = arrived[n, :PAD]
        left = jnp.where(place_col < ROWS, both[:, :DEEP].astype(F32), 0.0).astype(BF16)
        shifted = jnp.concatenate([both[:, ROWS:], jnp.zeros((PAD, DEEP - WIDE + ROWS), BF16)], axis=1)
        rest = dot_tn(arrived[n, PAD:, :PAD], pick)
        return left, (shifted.astype(F32) + rest).astype(BF16)

    packed[:, PAD:] = jnp.zeros((2, REST, WIDE), BF16)
    square = upper[:, :PAD]
    pack(0, jnp.where(square, diag[:PAD], diag[PAD:]), jnp.where(square, other_diag[:PAD], other_diag[PAD:]))
    swap = [remote(packed.at[n], arrived.at[n], z_send.at[n], z_recv.at[n], partner) for n in range(2)]
    swap[0].start()

    def meet_all(t, carry):
        meet(t)
        return carry

    lax.fori_loop(0, SHARED // 2, meet_all, 0)
    pack(1, cross[:PAD, :PAD], cross[PAD:, :PAD])
    swap[1].start()

    u_h = near[2 * SLOTS]
    u_o = near[2 * SLOTS + 1]
    diag_high, diag_low = halves(diag[...])
    alien_high, alien_low = halves(other_diag[...])
    cross_high, cross_low = halves(cross[...])
    x_h = dot(diag_high, u_h[:PAD]) + dot(diag_low, u_h[:PAD]) + (dot(cross_high, u_o) + dot(cross_low, u_o))
    x_o = dot(alien_high, u_o[:PAD]) + dot(alien_low, u_o[:PAD])
    flipped_high = jnp.concatenate([cross_high[:PAD], -cross_high[PAD:]], axis=1)
    flipped_low = jnp.concatenate([cross_low[:PAD], -cross_low[PAD:]], axis=1)
    x_o_turned = dot_tn(flipped_high, u_h[:PAD]) + dot_tn(flipped_low, u_h[:PAD])

    swap[0].wait_recv()
    theirs_own, theirs_other = unpack(0)
    plain, turned = unpacked_dots(theirs_own, upper, strict, u_o)
    x_o = x_o + plain
    x_o_turned = x_o_turned + turned
    plain, x_h_turned = unpacked_dots(theirs_other, upper, strict, u_h)
    x_h = x_h + plain

    swap[1].wait_recv()
    real, imag = unpack(1)
    x_h_turned = x_h_turned + dot_tn(jnp.concatenate([real, -imag], axis=1), u_o[:PAD])
    x_o = x_o + dot(jnp.concatenate([real, imag], axis=0), u_h)
    x_h = complex_rows(x_h, PAD, PAD) + complex_rows(x_h_turned, PAD, DEEP)
    x_o = complex_rows(x_o, PAD, PAD) + complex_rows(x_o_turned, PAD, DEEP)

    x_all = jnp.concatenate([x_h, x_o], axis=0)
    squares = jnp.sum(jnp.sum(x_all * x_all, axis=0, keepdims=True), axis=1, keepdims=True)
    scale = lax.rsqrt(2.0 * squares / HALF + 1e-06)
    gram = dot3(x_all, x_all, dot_tn) * (scale * scale)
    gram_real = gram[:HALF, :HALF] + gram[HALF:, HALF:]
    gram_imag = gram[:HALF, HALF:] - gram[HALF:, :HALF]
    eye = (
        lax.broadcasted_iota(jnp.int32, (HALF, HALF), 0) == lax.broadcasted_iota(jnp.int32, (HALF, HALF), 1)
    ).astype(F32)
    factor = stack_complex(1.5 * eye - 0.5 * gram_real, -0.5 * gram_imag)
    stacked = jnp.concatenate([x_h, jnp.concatenate([gram_real, gram_imag], axis=1)], axis=0)
    stacked = dot3(stacked, factor)
    gram = dot3(stacked[PAD:], factor)
    factor = stack_complex(1.5 * eye - 0.5 * gram[:, :HALF], -0.5 * gram[:, HALF:])
    out_ref[0] = (dot3(stacked[:PAD], factor) * (scale * math.sqrt(2.0 * ROWS)))[:ROWS]

    first.wait_send()
    for copy in sent + gifts + [tail_gift] + swap:
        copy.wait_send()
    for t in range(SHARED // 2):
        proj_copy(t).wait_send()


def on_device(margins, subspace, shell_weights, window_count):
    vmem = pl.BlockSpec(memory_space=pltpu.VMEM)
    smem = pl.BlockSpec(memory_space=pltpu.SMEM)
    return pl.pallas_call(
        kernel,
        out_shape=jax.ShapeDtypeStruct((1, ROWS, COLS), F32),
        in_specs=[smem, smem, pl.BlockSpec(memory_space=pl.ANY), pl.BlockSpec(memory_space=pl.ANY)],
        out_specs=vmem,
        scratch_shapes=[
            pltpu.VMEM((SHELL, ROWS, 4 * ROWS), BF16),
            pltpu.VMEM((GIFTS, ROWS, 4 * ROWS), BF16),
            pltpu.VMEM((ROWS, GIFTS * TAIL), BF16),
            pltpu.VMEM((ROWS, GIFTS * TAIL), BF16),
            pltpu.VMEM((2 * SHELL, 2 * PAD, DEEP), BF16),
            pltpu.VMEM((2 * SLOTS + 4, DEEP, COLS), BF16),
            pltpu.VMEM((SHARED, PAD, COLS), BF16),
            pltpu.VMEM((DEEP, COLS), BF16),
            pltpu.VMEM((2 * PAD, COLS), BF16),
            pltpu.VMEM((SHARED // 2, DEEP, COLS), BF16),
            pltpu.VMEM((2 * PAD, PAD), F32),
            pltpu.VMEM((2 * PAD, PAD), F32),
            pltpu.VMEM((2 * PAD, DEEP), F32),
            pltpu.VMEM((2, PAD + REST, WIDE), BF16),
            pltpu.VMEM((2, PAD + REST, WIDE), BF16),
            pltpu.SemaphoreType.DMA,
            pltpu.SemaphoreType.DMA((SLOTS + GIFTS,)),
            pltpu.SemaphoreType.DMA,
            pltpu.SemaphoreType.DMA,
            pltpu.SemaphoreType.DMA((GIFTS + 1,)),
            pltpu.SemaphoreType.DMA((GIFTS + 1,)),
            pltpu.SemaphoreType.DMA((2 * FAR + 2,)),
            pltpu.SemaphoreType.DMA((2 * FAR + 2,)),
            pltpu.SemaphoreType.DMA((SHARED // 2,)),
            pltpu.SemaphoreType.DMA((SHARED // 2,)),
            pltpu.SemaphoreType.DMA((2,)),
            pltpu.SemaphoreType.DMA((2,)),
        ],
        compiler_params=pltpu.CompilerParams(
            collective_id=0, has_side_effects=True, vmem_limit_bytes=60 * 1024 * 1024
        ),
        name="disentangle",
    )(window_count, shell_weights, margins[0], subspace)


def solution(mesh):
    return jax.shard_map(
        on_device,
        mesh=mesh,
        in_specs=(P("kpt", None, "band", None), P("kpt", "band", None), P(), P("kpt")),
        out_specs=P("kpt", "band", None),
        check_vma=False,
    )
```

```python
import functools
import math

import jax
import jax.numpy as jnp
from jax import lax
from jax.experimental import pallas as pl
from jax.experimental.pallas import tpu as pltpu
from jax.sharding import PartitionSpec as P

SIZE_X, SIZE_Y, SIZE_Z = 4, 4, 8
ROWS = 200
PAD = 208
DEEP = 256
COLS = 512
HALF = 256
SHELL = 12
GIFTS = 4
STEM = 768
TAIL = 4 * ROWS - STEM
WIDE = 384
REST = 2 * ROWS - WIDE
MESH = pl.DeviceIdType.MESH
F32 = jnp.float32
BF16 = jnp.bfloat16

SHARED = 4
SLOTS = 8
FAR = SLOTS + 1


def dot(a, b):
    return jnp.dot(a, b, preferred_element_type=F32)


def dot_nt(a, b):
    return lax.dot_general(a, b, (((1,), (1,)), ((), ())), preferred_element_type=F32)


def dot_tn(a, b):
    return lax.dot_general(a, b, (((0,), (0,)), ((), ())), preferred_element_type=F32)


def halves(a):
    high = a.astype(BF16)
    return high, (a - high.astype(F32)).astype(BF16)


def dot3(a, b, product=dot):
    a_high, a_low = halves(a)
    b_high, b_low = halves(b)
    return product(a_high, b_high) + (product(a_high, b_low) + product(a_low, b_high))


def combine(real, imag):
    return jnp.concatenate([real[:, :HALF] - imag[:, HALF:], real[:, HALF:] + imag[:, :HALF]], axis=1)


def complex_rows(both, rows, start):
    return combine(both[:rows], both[start:start + rows])


def stack_complex(real, imag):
    return jnp.concatenate(
        [jnp.concatenate([real, imag], axis=1), jnp.concatenate([-imag, real], axis=1)], axis=0
    )


def unpacked_dots(block, upper, strict, subspace):
    block = block.astype(F32)
    real = jnp.where(upper, block, 0.0).astype(BF16)
    above = jnp.where(strict, block, 0.0).astype(BF16)
    imag = jnp.where(upper, 0.0, block).astype(BF16)
    plain = dot(jnp.concatenate([real, imag], axis=0), subspace)
    turned = dot_tn(jnp.concatenate([above, -imag], axis=1), subspace[:PAD])
    return plain, turned


def kernel(
    window_ref, weight_ref, margin_ref, own_ref, out_ref,
    raw, spare, tails, given, split, near, mine, alien, rotated, theirs, diag, other_diag, cross, packed, arrived, lowered,
    own_sem, raw_sem, first_send, first_recv, gift_send, gift_recv, block_send, block_recv,
    proj_send, proj_recv, z_send, z_recv,
):
    kpt = lax.axis_index("kpt")
    band = lax.axis_index("band")
    other = 1 - band
    i = lax.div(kpt, SIZE_Y * SIZE_Z)
    j = lax.rem(lax.div(kpt, SIZE_Z), SIZE_Y)
    l = lax.rem(kpt, SIZE_Z)
    odd = lax.rem(l, 2)
    minus = lax.rem(band + odd + lax.div(l, 2), 2)
    sign = 1 - 2 * minus

    def point(di, dj, new_l):
        new_i = lax.rem(i + di + SIZE_X, SIZE_X)
        new_j = lax.rem(j + dj + SIZE_Y, SIZE_Y)
        return (new_i * SIZE_Y + new_j) * SIZE_Z + new_l

    l_near = l + 1 - 2 * odd
    l_far = lax.rem(l + 2 * odd - 1 + SIZE_Z, SIZE_Z)
    l_hop = lax.rem(l + 2 - 4 * odd + SIZE_Z, SIZE_Z)
    l_back = lax.rem(l - 2 + 4 * odd + SIZE_Z, SIZE_Z)

    takers = [
        (point(sign, 0, l_near), band), (point(-sign, 0, l_near), band),
        (point(0, sign, l_near), band),
    ]
    far_peer = (point(0, 0, l_far), other)
    far_takers = [(point(-sign, 0, l), band), (point(sign, 0, l), band)]
    hop_peer = (point(0, 0, l_hop), other)
    back_peer = (point(0, 0, l_back), other)
    partner = (kpt, other)

    plus = 1 - minus
    shell = [
        4 + 2 * minus + odd, 4 + 2 * plus + odd, 5 + 2 * minus - odd, 5 + 2 * plus - odd,
        8 + 2 * minus + odd, 1 + minus, 3 * plus, 9 + 2 * minus - odd,
    ]
    gift_shell = [8 + 2 * plus + odd, 1 + plus, 3 * minus, 9 + 2 * plus - odd]
    weights = [weight_ref[b] for b in shell]

    def weight_of(s):
        found = weights[0]
        for n in range(1, SLOTS):
            found = jnp.where(s == n, weights[n], found)
        return found

    loads = [
        pltpu.make_async_copy(margin_ref.at[shell[s]], raw.at[s], raw_sem.at[s]) for s in range(SLOTS)
    ]
    u_own = near.at[2 * SLOTS, pl.ds(0, ROWS)]
    own_load = pltpu.make_async_copy(own_ref.at[0], u_own, own_sem)
    own_load.start()
    gift_loads = [
        pltpu.make_async_copy(margin_ref.at[gift_shell[n]], spare.at[n], raw_sem.at[SLOTS + n]) for n in range(GIFTS)
    ]
    for load in loads + gift_loads:
        load.start()

    def clear(s, carry):
        near[s, ROWS:] = jnp.zeros((DEEP - ROWS, COLS), BF16)
        return carry

    lax.fori_loop(0, 2 * SLOTS + 2, clear, 0)
    theirs[:, ROWS:] = jnp.zeros((SHARED // 2, DEEP - ROWS, COLS), BF16)

    barrier = pltpu.get_barrier_semaphore()
    peers = takers + far_takers + [far_peer, hop_peer, back_peer, partner]
    for peer in peers:
        pl.semaphore_signal(barrier, inc=1, device_id=peer, device_id_type=MESH)
    pl.semaphore_wait(barrier, len(peers))

    def remote(src, dst, send_sem, recv_sem, peer):
        return pltpu.make_async_remote_copy(
            src_ref=src, dst_ref=dst, send_sem=send_sem, recv_sem=recv_sem, device_id=peer, device_id_type=MESH
        )

    def block(s, q):
        return near.at[2 * s + q, pl.ds(0, ROWS)]

    def wait_block(s, q):
        remote(block(s, q), block(s, q), block_send.at[0], block_recv.at[2 * s + q], partner).wait_recv()

    u_other = near.at[2 * SLOTS + 1, pl.ds(0, ROWS)]
    sent = []

    def pass_on(src, s, q, turn, peer):
        copy = remote(src, block(s, q), block_send.at[2 * s + turn], block_recv.at[2 * s + q], peer)
        copy.start()
        sent.append(copy)

    first = remote(u_own, u_other, first_send, first_recv, partner)
    own_load.wait()
    first.start()
    def offer(src, q, turn):
        pass_on(src, 4, q, turn, takers[2])
        pass_on(src, FAR, q, turn, far_peer)
        for s in (0, 1):
            pass_on(src, s, q, turn, takers[s])

    offer(u_own, band, 0)
    gifts = [
        remote(
            margin_ref.at[gift_shell[n], :, pl.ds(0, STEM)], raw.at[SLOTS + n, :, pl.ds(0, STEM)], gift_send.at[n],
            gift_recv.at[n], partner,
        )
        for n in range(GIFTS)
    ]
    tail_gift = remote(tails, given, gift_send.at[GIFTS], gift_recv.at[GIFTS], partner)

    diag[...] = jnp.zeros_like(diag)
    other_diag[...] = jnp.zeros_like(other_diag)
    cross[...] = jnp.zeros_like(cross)
    split[...] = jnp.zeros_like(split)
    for load in loads + gift_loads:
        load.wait()
    for n in range(GIFTS):
        tails[:, n * TAIL:(n + 1) * TAIL] = spare[n, :, STEM:]

    def separate(s, carry):
        whole = raw[s]
        for part in range(4):
            piece = whole[:, part * ROWS:(part + 1) * ROWS]
            split[2 * s + part % 2, (part // 2) * PAD:(part // 2) * PAD + ROWS, :ROWS] = piece
        return carry

    gifts[0].start()
    lax.fori_loop(0, 4, separate, 0)
    tail_gift.start()
    for gift in gifts[1:]:
        gift.start()

    first.wait_recv()
    offer(u_other, other, 1)

    for turn, q in enumerate((band, other)):
        wait_block(FAR, q)
        for n in range(2):
            pass_on(block(FAR, q), 2 + n, q, turn, far_takers[n])
        wait_block(4, q)
        for n in range(2):
            pass_on(block(4, q), 5 + n, q, turn, takers[n])
        pass_on(block(4, q), 7, q, turn, hop_peer)
        if turn == 0:
            lax.fori_loop(4, SLOTS, separate, 0)

    row = lax.broadcasted_iota(jnp.int32, (PAD, 1), 0)

    def projection(margin, s, owner):
        both = dot(split[2 * margin], near[2 * s]) + dot(split[2 * margin + 1], near[2 * s + 1])
        inside = (row < ROWS) & (row + owner * ROWS < window_ref[0])
        return jnp.where(inside, complex_rows(both, PAD, PAD), 0.0).astype(BF16)

    def turn_by(projected):
        rotated[0:PAD] = projected
        rotated[PAD:, :HALF] = projected[:, HALF:]
        rotated[PAD:, HALF:] = -projected[:, :HALF]

    def project(s, carry):
        projected = projection(s, s, band)
        mine[s] = projected
        turn_by(projected)
        diag[...] += weight_of(s) * dot_nt(rotated[...], projected)
        return carry

    def project_all(s, carry):
        aliens = projection(s + GIFTS, s, other)
        weight = weight_of(s)
        turn_by(aliens)
        other_diag[...] += weight * dot_nt(rotated[...], aliens)
        alien[0:PAD] = aliens
        projected = projection(s, s, band)
        turn_by(projected)
        diag[...] += weight * dot_nt(rotated[...], projected)
        cross[...] += weight * dot_nt(rotated[...], alien[...])
        return carry

    def proj_copy(t):
        return remote(
            mine.at[2 * t, pl.ds(0, ROWS)], theirs.at[t, pl.ds(0, ROWS)], proj_send.at[t], proj_recv.at[t], partner
        )

    def meet(t):
        proj_copy(t).wait_recv()
        turn_by(mine[2 * t + 1])
        cross[...] += weight_of(2 * t + 1) * dot_nt(rotated[...], theirs[t])

    alien[PAD:] = jnp.zeros((DEEP - PAD, COLS), BF16)

    def pair(t, carry):
        lax.fori_loop(2 * t, 2 * t + 2, project, 0)
        proj_copy(t).start()
        return carry

    def wait_pair(t, carry):
        for u in range(2):
            for q in range(2):
                wait_block(2 * t + u, q)
        return carry

    def shared(t, carry):
        wait_pair(t, 0)
        return pair(t, carry)

    def swapped(n, carry):
        stem = raw.at[SLOTS + n, :, pl.ds(0, STEM)]
        remote(stem, stem, gift_send.at[n], gift_recv.at[n], partner).wait_recv()
        separate(SLOTS + n, 0)

        @pl.when(n > 0)
        def _():
            for q in range(2):
                wait_block(SHARED + n, q)

        project_all(SHARED + n, 0)
        return carry

    lax.fori_loop(0, SHARED // 2, shared, 0)
    tail_gift.wait_recv()
    for n in range(GIFTS):
        raw[SLOTS + n, :, STEM:] = given[:, n * TAIL:(n + 1) * TAIL]
    lax.fori_loop(0, GIFTS, swapped, 0)

    place_row = lax.broadcasted_iota(jnp.int32, (PAD, DEEP), 0)
    place_col = lax.broadcasted_iota(jnp.int32, (PAD, DEEP), 1)
    upper = place_row <= place_col
    strict = place_row < place_col
    pick = (
        lax.broadcasted_iota(jnp.int32, (REST, DEEP), 1) == ROWS - REST + lax.broadcasted_iota(jnp.int32, (REST, DEEP), 0)
    ).astype(BF16)

    def pack(n, left, right):
        left, right = left.astype(BF16), right.astype(BF16)
        packed[n, :PAD] = jnp.concatenate([left[:, :ROWS], right[:, :ROWS - REST]], axis=1)
        packed[n, PAD:, :PAD] = dot_nt(pick[:, :PAD], right).astype(BF16)

    def unpack(n):
        both = arrived[n, :PAD]
        left = jnp.where(place_col < ROWS, both[:, :DEEP].astype(F32), 0.0).astype(BF16)
        shifted = jnp.concatenate([both[:, ROWS:], jnp.zeros((PAD, DEEP - WIDE + ROWS), BF16)], axis=1)
        rest = dot_tn(arrived[n, PAD:, :PAD], pick)
        return left, (shifted.astype(F32) + rest).astype(BF16)

    packed[:, PAD:] = jnp.zeros((2, REST, WIDE), BF16)
    square = upper[:, :PAD]
    pack(0, jnp.where(square, diag[:PAD], diag[PAD:]), jnp.where(square, other_diag[:PAD], other_diag[PAD:]))
    swap = [remote(packed.at[n], arrived.at[n], z_send.at[n], z_recv.at[n], partner) for n in range(2)]
    swap[0].start()

    def meet_all(t, carry):
        meet(t)
        return carry

    lax.fori_loop(0, SHARED // 2, meet_all, 0)
    pack(1, cross[:PAD, :PAD], cross[PAD:, :PAD])
    swap[1].start()

    u_h = near[2 * SLOTS]
    u_o = near[2 * SLOTS + 1]
    diag_high, diag_low = halves(diag[...])
    alien_high, alien_low = halves(other_diag[...])
    cross_high, cross_low = halves(cross[...])
    x_h = dot(diag_high, u_h[:PAD]) + dot(diag_low, u_h[:PAD]) + (dot(cross_high, u_o) + dot(cross_low, u_o))
    x_o = dot(alien_high, u_o[:PAD]) + dot(alien_low, u_o[:PAD])
    flipped_high = jnp.concatenate([cross_high[:PAD], -cross_high[PAD:]], axis=1)
    flipped_low = jnp.concatenate([cross_low[:PAD], -cross_low[PAD:]], axis=1)
    x_o_turned = dot_tn(flipped_high, u_h[:PAD]) + dot_tn(flipped_low, u_h[:PAD])

    lowered[:ROWS] = jnp.zeros((ROWS, COLS), BF16)
    lowered[ROWS:] = u_h[:ROWS]

    swap[0].wait_recv()
    theirs_own, theirs_other = unpack(0)
    plain, turned = unpacked_dots(theirs_own, upper, strict, u_o)
    x_o = x_o + plain
    x_o_turned = x_o_turned + turned
    plain, x_h_turned = unpacked_dots(theirs_other, upper, strict, u_h)
    x_h = x_h + plain

    x_h = complex_rows(x_h, PAD, PAD) + complex_rows(x_h_turned, PAD, DEEP)
    x_o = complex_rows(x_o, PAD, PAD) + complex_rows(x_o_turned, PAD, DEEP)

    swap[1].wait_recv()
    both, rest = arrived[1, :PAD], arrived[1, PAD:, :PAD]
    x_o = x_o + combine(dot(both[:, :DEEP], u_h), dot(both, lowered[:WIDE]) + dot_tn(rest, lowered[WIDE:]))
    turned = dot_tn(both, u_o[:PAD])
    imag = jnp.concatenate([turned[ROWS:], dot(rest, u_o[:PAD])], axis=0)
    x_h = x_h + jnp.concatenate([combine(turned[:ROWS], -imag), jnp.zeros((PAD - ROWS, COLS), F32)], axis=0)

    x_all = jnp.concatenate([x_h, x_o], axis=0)
    squares = jnp.sum(jnp.sum(x_all * x_all, axis=0, keepdims=True), axis=1, keepdims=True)
    scale = lax.rsqrt(2.0 * squares / HALF + 1e-06)
    gram = dot3(x_all, x_all, dot_tn) * (scale * scale)
    gram_real = gram[:HALF, :HALF] + gram[HALF:, HALF:]
    gram_imag = gram[:HALF, HALF:] - gram[HALF:, :HALF]
    eye = (
        lax.broadcasted_iota(jnp.int32, (HALF, HALF), 0) == lax.broadcasted_iota(jnp.int32, (HALF, HALF), 1)
    ).astype(F32)
    factor = stack_complex(1.5 * eye - 0.5 * gram_real, -0.5 * gram_imag)
    stacked = jnp.concatenate([x_h, jnp.concatenate([gram_real, gram_imag], axis=1)], axis=0)
    stacked = dot3(stacked, factor)
    gram = dot3(stacked[PAD:], factor)
    factor = stack_complex(1.5 * eye - 0.5 * gram[:, :HALF], -0.5 * gram[:, HALF:])
    out_ref[0] = (dot3(stacked[:PAD], factor) * (scale * math.sqrt(2.0 * ROWS)))[:ROWS]

    first.wait_send()
    for copy in sent + gifts + [tail_gift] + swap:
        copy.wait_send()
    for t in range(SHARED // 2):
        proj_copy(t).wait_send()


def on_device(margins, subspace, shell_weights, window_count):
    vmem = pl.BlockSpec(memory_space=pltpu.VMEM)
    smem = pl.BlockSpec(memory_space=pltpu.SMEM)
    return pl.pallas_call(
        kernel,
        out_shape=jax.ShapeDtypeStruct((1, ROWS, COLS), F32),
        in_specs=[smem, smem, pl.BlockSpec(memory_space=pl.ANY), pl.BlockSpec(memory_space=pl.ANY)],
        out_specs=vmem,
        scratch_shapes=[
            pltpu.VMEM((SHELL, ROWS, 4 * ROWS), BF16),
            pltpu.VMEM((GIFTS, ROWS, 4 * ROWS), BF16),
            pltpu.VMEM((ROWS, GIFTS * TAIL), BF16),
            pltpu.VMEM((ROWS, GIFTS * TAIL), BF16),
            pltpu.VMEM((2 * SHELL, 2 * PAD, DEEP), BF16),
            pltpu.VMEM((2 * SLOTS + 4, DEEP, COLS), BF16),
            pltpu.VMEM((SHARED, PAD, COLS), BF16),
            pltpu.VMEM((DEEP, COLS), BF16),
            pltpu.VMEM((2 * PAD, COLS), BF16),
            pltpu.VMEM((SHARED // 2, DEEP, COLS), BF16),
            pltpu.VMEM((2 * PAD, PAD), F32),
            pltpu.VMEM((2 * PAD, PAD), F32),
            pltpu.VMEM((2 * PAD, DEEP), F32),
            pltpu.VMEM((2, PAD + REST, WIDE), BF16),
            pltpu.VMEM((2, PAD + REST, WIDE), BF16),
            pltpu.VMEM((2 * ROWS, COLS), BF16),
            pltpu.SemaphoreType.DMA,
            pltpu.SemaphoreType.DMA((SLOTS + GIFTS,)),
            pltpu.SemaphoreType.DMA,
            pltpu.SemaphoreType.DMA,
            pltpu.SemaphoreType.DMA((GIFTS + 1,)),
            pltpu.SemaphoreType.DMA((GIFTS + 1,)),
            pltpu.SemaphoreType.DMA((2 * FAR + 2,)),
            pltpu.SemaphoreType.DMA((2 * FAR + 2,)),
            pltpu.SemaphoreType.DMA((SHARED // 2,)),
            pltpu.SemaphoreType.DMA((SHARED // 2,)),
            pltpu.SemaphoreType.DMA((2,)),
            pltpu.SemaphoreType.DMA((2,)),
        ],
        compiler_params=pltpu.CompilerParams(
            collective_id=0, has_side_effects=True, vmem_limit_bytes=60 * 1024 * 1024
        ),
        name="disentangle",
    )(window_count, shell_weights, margins[0], subspace)


def solution(mesh):
    return jax.shard_map(
        on_device,
        mesh=mesh,
        in_specs=(P("kpt", None, "band", None), P("kpt", "band", None), P(), P("kpt")),
        out_specs=P("kpt", "band", None),
        check_vma=False,
    )
```
